32 devices in a mesh: scen: 16 (over z, y, x), fac: 2 (over core).
Axes of the slice: x: 2, y: 2, z: 4, core: 2. Of those that a mesh axis runs over, the one named last changes fastest.
Arguments:
- scenarios: bfloat16 [256, 8192], P(('scen', 'fac')), may hold values from -40 to 40
Outputs:
- shrunk: float32 [8192, 8192], P('scen', 'fac')
- shrinkage: float32 [], replicated
- col_mean: float32 [8192], P('fac')
The draws below stay inside these ranges and needn't reach their ends.
All inputs are finite; a program needn't handle non-finite values.
Results may differ from the reference program's by a relative error of at most 0.0008.
Values may be sent and summed in bfloat16 or wider, within the bound.
A program may use at most 64 MiB of HBM per device.

```python
import math
import jax
import jax.numpy as jnp
from jax import lax

FACTORS = 8192
SCENARIOS = 256


def draw_scenarios(key, part):
    keys = jax.random.split(key, 3)
    offsets = jax.random.uniform(keys[0], (FACTORS,), jnp.float32, -12.0, 12.0)
    position = jnp.arange(SCENARIOS, dtype=jnp.float32) / (SCENARIOS - 1)
    ramp = 0.5 + position
    row_scale = 0.6 + 1.2 * position
    scales = jnp.exp(jax.random.uniform(keys[1], (FACTORS,), jnp.float32, math.log(0.3), math.log(3.0)))
    noise = jnp.clip(jax.random.normal(keys[2], (SCENARIOS, FACTORS), jnp.float32), -4.0, 4.0)
    values = offsets * ramp[:, None] + scales * row_scale[:, None] * noise
    return jnp.clip(values, -40.0, 40.0).astype(jnp.bfloat16)


def setup_inputs(seed: int = 0) -> dict:
    arg_keys = jax.random.split(jax.random.key(seed), 2)
    scenarios = draw_scenarios(jax.random.fold_in(arg_keys[1], 71), 0)
    return dict(scenarios=scenarios)


def reference(scenarios):
    values = scenarios.astype(jnp.float32)
    col_mean = jnp.sum(values, axis=0) / SCENARIOS
    centered = (values - col_mean).astype(jnp.bfloat16)
    as_float = centered.astype(jnp.float32)
    squared = jnp.sum(as_float * as_float, axis=1)
    trace_total = jnp.sum(squared)
    fourth_total = jnp.sum(squared * squared)
    covariance = jnp.dot(as_float.T, as_float, precision=lax.Precision.HIGHEST) / SCENARIOS
    mu_scale = trace_total / (SCENARIOS * FACTORS)
    diag_mask = jnp.eye(FACTORS, dtype=jnp.float32)
    distance = covariance - mu_scale * diag_mask
    spread = jnp.sum(distance * distance) / FACTORS
    norm_sq = FACTORS * (spread + mu_scale * mu_scale)
    beta_value = (fourth_total / SCENARIOS - norm_sq) / (FACTORS * SCENARIOS)
    shrinkage = beta_value / spread
    shrunk = (1.0 - shrinkage) * covariance + shrinkage * mu_scale * diag_mask
    return shrunk, shrinkage, col_mean
```

```python
import functools

import jax
import jax.numpy as jnp
from jax import lax
from jax.experimental import pallas as pl
from jax.experimental.pallas import tpu as pltpu
from jax.sharding import PartitionSpec as P

MESH = pl.DeviceIdType.MESH
F32 = jnp.float32
BF16 = jnp.bfloat16


def gather_kernel(lines, rows_ref, mine_ref, other_ref, local_sem, pair_sems, z_sems, x_sems, y_sems, d_sems, core_sems):
    scen = lax.axis_index("scen")
    fac = lax.axis_index("fac")
    z, y, x = scen // 4, (scen // 2) % 2, scen % 2
    half = mine_ref.shape[-1]
    mid = half // 2

    def chip(k, yy, xx):
        return k * 4 + yy * 2 + xx

    x_next = (chip(z, y, 1 - x), fac)
    y_next = (chip(z, 1 - y, x), fac)
    partner = (scen, 1 - fac)
    above = (chip(jnp.minimum(z + 1, lines - 1), y, x), fac)
    below = (chip(jnp.maximum(z - 1, 0), y, x), fac)
    has_above = z < lines - 1
    has_below = z > 0

    barrier = pltpu.get_barrier_semaphore()
    for device in (x_next, y_next, partner):
        pl.semaphore_signal(barrier, inc=1, device_id=device, device_id_type=MESH)

    @pl.when(has_above)
    def _():
        pl.semaphore_signal(barrier, inc=1, device_id=above, device_id_type=MESH)

    @pl.when(has_below)
    def _():
        pl.semaphore_signal(barrier, inc=1, device_id=below, device_id_type=MESH)

    pl.semaphore_wait(barrier, 3 + has_above.astype(jnp.int32) + has_below.astype(jnp.int32))

    def copy(src, dst, sems, i, device):
        return pltpu.make_async_remote_copy(
            src_ref=src, dst_ref=dst, send_sem=sems.at[0, i], recv_sem=sems.at[1, i], device_id=device, device_id_type=MESH
        )

    def block(c):
        return mine_ref.at[c]

    keep = pltpu.make_async_copy(rows_ref.at[:, pl.ds(pl.multiple_of(fac * half, half), half)], mine_ref.at[scen, fac], local_sem.at[0])
    keep.start()
    give = copy(
        rows_ref.at[:, pl.ds(pl.multiple_of((1 - fac) * half, half), half)], mine_ref.at[scen, fac], pair_sems, 0, partner
    )
    give.start()
    keep.wait()
    give.wait_recv()

    def up(k):
        return copy(block(chip(k, y, x)), block(chip(k, y, x)), z_sems, k, above)

    def down(k):
        return pltpu.make_async_remote_copy(
            src_ref=block(chip(k, y, x)),
            dst_ref=block(chip(k, y, x)),
            send_sem=z_sems.at[2, k],
            recv_sem=z_sems.at[1, k],
            device_id=below,
            device_id_type=MESH,
        )

    def to_x(k):
        return copy(block(chip(k, y, x)), block(chip(k, y, x)), x_sems, k, x_next)

    def to_y(k):
        return copy(block(chip(k, y, x)), block(chip(k, y, x)), y_sems, k, y_next)

    def part(c, i):
        return mine_ref.at[c, :, :, pl.ds(i * mid, mid)]

    def diag_x(k):
        c = chip(k, 1 - y, x)
        return copy(part(c, 0), part(c, 0), d_sems, 2 * k, x_next)

    def diag_y(k):
        c = chip(k, y, 1 - x)
        return copy(part(c, 1), part(c, 1), d_sems, 2 * k + 1, y_next)

    def to_core(c):
        return copy(mine_ref.at[c], other_ref.at[c], core_sems, c, partner)

    def line_step(k, ups, downs, arrived):
        if arrived:
            up(k).wait_recv()
        to_x(k).start()
        to_y(k).start()
        if ups:
            @pl.when(has_above)
            def _():
                up(k).start()
        if downs:
            @pl.when(has_below)
            def _():
                down(k).start()
        to_core(chip(k, y, x)).start()

    def side_step(k):
        to_x(k).wait_recv()
        diag_y(k).start()
        to_core(chip(k, y, 1 - x)).start()
        to_y(k).wait_recv()
        diag_x(k).start()
        to_core(chip(k, 1 - y, x)).start()

    def diag_step(k):
        diag_x(k).wait_recv()
        diag_y(k).wait_recv()
        to_core(chip(k, 1 - y, 1 - x)).start()

    def each(d, step):
        if d == 0:
            step(z, 0)
            return

        @pl.when(z - d >= 0)
        def _():
            step(z - d, -1)

        @pl.when(z + d < lines)
        def _():
            step(z + d, 1)

    line_step(z, True, True, False)
    for d in range(1, lines):
        each(d, lambda k, sign: line_step(k, sign < 0, sign > 0, True))
        each(d - 1, lambda k, sign: side_step(k))
    each(lines - 1, lambda k, sign: side_step(k))
    for d in range(lines):
        each(d, lambda k, sign: diag_step(k))

    give.wait_send()
    for k in range(lines):
        to_x(k).wait_send()
        to_y(k).wait_send()
        diag_x(k).wait_send()
        diag_y(k).wait_send()

        @pl.when((k <= z) & has_above)
        def _():
            up(k).wait_send()

        @pl.when((k >= z) & has_below)
        def _():
            down(k).wait_send()
    for c in range(4 * lines):
        to_core(c).wait()


def shrink_kernel(steps, mine_ref, other_ref, out_ref, shrinkage_ref, mean_ref, cols, cols_other, narrow, scalars):
    step = pl.program_id(0)
    scen = lax.axis_index("scen")
    fac = lax.axis_index("fac")
    blocks, rows, half = mine_ref.shape
    total_rows = blocks * rows
    factors = 2 * half
    width = narrow.shape[0]
    tall = out_ref.shape[0]
    per_half = half // width
    in_mine = scen // per_half == fac
    offset = (scen % per_half) * width

    @pl.when(step == 0)
    def _():
        chunk = 512

        def centre(src, dst, i, mean_out):
            at = pl.ds(pl.multiple_of(i * chunk, chunk), chunk)
            total = src[0, :, at].astype(F32)
            for j in range(1, blocks):
                total = total + src[j, :, at].astype(F32)
            mean = jnp.sum(total, axis=0, keepdims=True) / total_rows
            if mean_out is not None:
                mean_out[:, at] = mean
            for j in range(0, blocks, 2):
                pair = src[pl.ds(j, 2), :, at].astype(F32).reshape(2 * rows, chunk)
                dst[pl.ds(j * rows, 2 * rows), at] = (pair - mean).astype(BF16)

        @pl.loop(0, half // chunk)
        def _(i):
            centre(mine_ref, cols, i, mean_ref)
            centre(other_ref, cols_other, i, None)

        at = pl.ds(pl.multiple_of(offset, width), width)

        @pl.when(in_mine)
        def _():
            narrow[...] = cols[:, at].T

        @pl.when(jnp.logical_not(in_mine))
        def _():
            narrow[...] = cols_other[:, at].T

        across = (((1,), (1,)), ((), ()))
        gram = lax.dot_general(cols[...], cols[...], across, preferred_element_type=F32)
        gram = gram + lax.dot_general(cols_other[...], cols_other[...], across, preferred_element_type=F32)
        on_diag = lax.broadcasted_iota(jnp.int32, gram.shape, 0) == lax.broadcasted_iota(jnp.int32, gram.shape, 1)
        gram_sq = gram * gram

        def total_of(v):
            return jnp.sum(jnp.sum(v, axis=0, keepdims=True), axis=1, keepdims=True)

        trace_total = total_of(jnp.where(on_diag, gram, 0.0))
        fourth_total = total_of(jnp.where(on_diag, gram_sq, 0.0))
        cov_sq = total_of(gram_sq) / (total_rows * total_rows)
        mu_scale = trace_total / (total_rows * factors)
        spread = (cov_sq - factors * mu_scale * mu_scale) / factors
        norm_sq = factors * (spread + mu_scale * mu_scale)
        beta_value = (fourth_total / total_rows - norm_sq) / (factors * total_rows)
        shrinkage = beta_value / spread
        shrinkage_ref[...] = shrinkage
        scalars[0:1, :] = jnp.broadcast_to((1.0 - shrinkage) / total_rows, (1, 128))
        scalars[1:2, :] = jnp.broadcast_to(shrinkage * mu_scale, (1, 128))

    scale = scalars[0:1, 0:1]
    left = narrow[pl.ds(pl.multiple_of(step * tall, tall), tall), :]
    piece = 1024
    for i in range(half // piece):
        at = pl.ds(i * piece, piece)
        out_ref[:, at] = jnp.dot(left, cols[:, at], preferred_element_type=F32) * scale

    @pl.when(in_mine)
    def _():
        at = pl.ds(pl.multiple_of(offset + step * tall, tall), tall)
        eye = lax.broadcasted_iota(jnp.int32, (tall, tall), 0) == lax.broadcasted_iota(jnp.int32, (tall, tall), 1)
        out_ref[:, at] = out_ref[:, at] + jnp.where(eye, scalars[1:2, 0:1], 0.0)


def on_chip_pairs(scenarios):
    rows, factors = scenarios.shape
    scen_size = lax.axis_size("scen")
    fac_size = lax.axis_size("fac")
    lines = scen_size // 4
    half = factors // fac_size
    width = factors // scen_size
    vmem = pl.BlockSpec(memory_space=pltpu.VMEM)
    held = jax.ShapeDtypeStruct((scen_size, 2, rows, half), BF16)
    dma = pltpu.SemaphoreType.DMA
    mine, other = pl.pallas_call(
        functools.partial(gather_kernel, lines),
        out_shape=(held, held),
        in_specs=[vmem],
        out_specs=(vmem, vmem),
        scratch_shapes=[
            dma((1,)),
            dma((2, 1)),
            dma((3, lines)),
            dma((2, lines)),
            dma((2, lines)),
            dma((2, 2 * lines)),
            dma((2, scen_size)),
        ],
        compiler_params=pltpu.CompilerParams(collective_id=0, has_side_effects=True),
        name="gather_rows",
    )(scenarios)
    mine = mine.reshape(2 * scen_size, rows, half)
    other = other.reshape(2 * scen_size, rows, half)
    total_rows = 2 * scen_size * rows
    tall = 128
    steps = width // tall
    shrunk, shrinkage, mean_block = pl.pallas_call(
        functools.partial(shrink_kernel, steps),
        grid=(steps,),
        out_shape=(
            jax.ShapeDtypeStruct((width, half), F32),
            jax.ShapeDtypeStruct((1, 1), F32),
            jax.ShapeDtypeStruct((1, half), F32),
        ),
        in_specs=[vmem, vmem],
        out_specs=(
            pl.BlockSpec((tall, half), lambda i: (i, 0)),
            pl.BlockSpec((1, 1), lambda i: (0, 0)),
            pl.BlockSpec((1, half), lambda i: (0, 0)),
        ),
        scratch_shapes=[
            pltpu.VMEM((total_rows, half), BF16),
            pltpu.VMEM((total_rows, half), BF16),
            pltpu.VMEM((width, total_rows), BF16),
            pltpu.VMEM((8, 128), F32),
        ],
        compiler_params=pltpu.CompilerParams(dimension_semantics=("arbitrary",)),
        name="shrink_rows",
    )(mine, other)
    return shrunk, shrinkage.reshape(()), mean_block.reshape(half)


def on_device(scenarios):
    row_count = scenarios.shape[0]
    factors = scenarios.shape[1]
    scen_size = lax.axis_size("scen")
    fac_size = lax.axis_size("fac")
    total_rows = row_count * scen_size * fac_size
    group_width = factors // scen_size
    block_width = factors // fac_size
    owner_idx = lax.axis_index("scen")
    block_idx = lax.axis_index("fac")
    col_total = lax.psum(jnp.sum(scenarios.astype(jnp.float32), axis=0), ("scen", "fac"))
    col_mean = col_total / total_rows
    centered = (scenarios.astype(jnp.float32) - col_mean).astype(jnp.bfloat16)
    as_float = centered.astype(jnp.float32)
    squared = jnp.sum(as_float * as_float, axis=1)
    trace_part = jnp.sum(squared)
    fourth_part = jnp.sum(squared * squared)
    trace_total, fourth_total = lax.psum((trace_part, fourth_part), ("scen", "fac"))
    contract = (((0,), (0,)), ((), ()))
    local_rows = lax.all_gather(centered, "fac", axis=0, tiled=True)
    narrow_all = lax.all_to_all(local_rows, "scen", split_axis=1, concat_axis=0, tiled=True)
    wide_cols = lax.dynamic_slice_in_dim(local_rows, block_idx * block_width, block_width, 1)
    summed = lax.dot_general(
        narrow_all,
        lax.all_gather(wide_cols, "scen", axis=0, tiled=True),
        contract,
        preferred_element_type=jnp.float32,
    )
    covariance = summed / total_rows
    row_index = owner_idx * group_width + lax.broadcasted_iota(
        jnp.int32, (group_width, block_width), 0
    )
    col_index = block_idx * block_width + lax.broadcasted_iota(
        jnp.int32, (group_width, block_width), 1
    )
    diag_mask = (row_index == col_index).astype(jnp.float32)
    mu_scale = trace_total / (total_rows * factors)
    distance = covariance - mu_scale * diag_mask
    frob_sum = lax.psum(jnp.sum(distance * distance), ("scen", "fac"))
    spread = frob_sum / factors
    norm_sq = factors * (spread + mu_scale * mu_scale)
    beta_value = (fourth_total / total_rows - norm_sq) / (factors * total_rows)
    shrinkage = beta_value / spread
    shrunk = (1.0 - shrinkage) * covariance + shrinkage * mu_scale * diag_mask
    mean_block = lax.dynamic_slice_in_dim(col_mean, block_idx * block_width, block_width, 0)
    return (shrunk, shrinkage, mean_block)


def solution(mesh):
    pairs = mesh.shape["fac"] == 2 and mesh.shape["scen"] % 4 == 0

    def step(scenarios):
        rows, factors = scenarios.shape
        width = factors // lax.axis_size("scen")
        gathered = rows * lax.axis_size("scen") * factors * 2 * scenarios.dtype.itemsize
        if pairs and rows == 8 and width % 128 == 0 and (factors // 2) % 1024 == 0 and gathered <= 2**23:
            return on_chip_pairs(scenarios)
        return on_device(scenarios)

    return jax.shard_map(
        step,
        mesh=mesh,
        in_specs=(P(("scen", "fac"), None),),
        out_specs=(P("scen", "fac"), P(), P("fac")),
        check_vma=False,
    )
```

```python
import functools

import jax
import jax.numpy as jnp
from jax import lax
from jax.experimental import pallas as pl
from jax.experimental.pallas import tpu as pltpu
from jax.sharding import PartitionSpec as P

MESH = pl.DeviceIdType.MESH
F32 = jnp.float32
BF16 = jnp.bfloat16


def gather_kernel(lines, rows_ref, mine_ref, other_ref, local_sem, pair_sems, z_sems, x_sems, y_sems, d_sems, core_sems):
    scen = lax.axis_index("scen")
    fac = lax.axis_index("fac")
    z, y, x = scen // 4, (scen // 2) % 2, scen % 2
    half = mine_ref.shape[-1]
    mid = half // 2

    def chip(k, yy, xx):
        return k * 4 + yy * 2 + xx

    x_next = (chip(z, y, 1 - x), fac)
    y_next = (chip(z, 1 - y, x), fac)
    partner = (scen, 1 - fac)
    above = (chip(jnp.minimum(z + 1, lines - 1), y, x), fac)
    below = (chip(jnp.maximum(z - 1, 0), y, x), fac)
    has_above = z < lines - 1
    has_below = z > 0

    barrier = pltpu.get_barrier_semaphore()
    for device in (x_next, y_next, partner):
        pl.semaphore_signal(barrier, inc=1, device_id=device, device_id_type=MESH)

    @pl.when(has_above)
    def _():
        pl.semaphore_signal(barrier, inc=1, device_id=above, device_id_type=MESH)

    @pl.when(has_below)
    def _():
        pl.semaphore_signal(barrier, inc=1, device_id=below, device_id_type=MESH)

    pl.semaphore_wait(barrier, 3 + has_above.astype(jnp.int32) + has_below.astype(jnp.int32))

    def copy(src, dst, sems, i, device):
        return pltpu.make_async_remote_copy(
            src_ref=src, dst_ref=dst, send_sem=sems.at[0, i], recv_sem=sems.at[1, i], device_id=device, device_id_type=MESH
        )

    def block(c):
        return mine_ref.at[c]

    keep = pltpu.make_async_copy(rows_ref.at[:, pl.ds(pl.multiple_of(fac * half, half), half)], mine_ref.at[scen, fac], local_sem.at[0])
    keep.start()
    give = copy(
        rows_ref.at[:, pl.ds(pl.multiple_of((1 - fac) * half, half), half)], mine_ref.at[scen, fac], pair_sems, 0, partner
    )
    give.start()
    keep.wait()
    give.wait_recv()

    def up(k):
        return copy(block(chip(k, y, x)), block(chip(k, y, x)), z_sems, k, above)

    def down(k):
        return pltpu.make_async_remote_copy(
            src_ref=block(chip(k, y, x)),
            dst_ref=block(chip(k, y, x)),
            send_sem=z_sems.at[2, k],
            recv_sem=z_sems.at[1, k],
            device_id=below,
            device_id_type=MESH,
        )

    def to_x(k):
        return copy(block(chip(k, y, x)), block(chip(k, y, x)), x_sems, k, x_next)

    def to_y(k):
        return copy(block(chip(k, y, x)), block(chip(k, y, x)), y_sems, k, y_next)

    def part(c, i):
        return mine_ref.at[c, :, :, pl.ds(i * mid, mid)]

    def diag_x(k):
        c = chip(k, 1 - y, x)
        return copy(part(c, 0), part(c, 0), d_sems, 2 * k, x_next)

    def diag_y(k):
        c = chip(k, y, 1 - x)
        return copy(part(c, 1), part(c, 1), d_sems, 2 * k + 1, y_next)

    def to_core(c):
        return copy(mine_ref.at[c], other_ref.at[c], core_sems, c, partner)

    def line_step(k, ups, downs, arrived):
        if arrived:
            up(k).wait_recv()
        to_x(k).start()
        to_y(k).start()
        if ups:
            @pl.when(has_above)
            def _():
                up(k).start()
        if downs:
            @pl.when(has_below)
            def _():
                down(k).start()
        to_core(chip(k, y, x)).start()

    def side_step(k):
        to_x(k).wait_recv()
        diag_y(k).start()
        to_core(chip(k, y, 1 - x)).start()
        to_y(k).wait_recv()
        diag_x(k).start()
        to_core(chip(k, 1 - y, x)).start()

    def diag_step(k):
        diag_x(k).wait_recv()
        diag_y(k).wait_recv()
        to_core(chip(k, 1 - y, 1 - x)).start()

    def each(d, step):
        if d == 0:
            step(z, 0)
            return

        @pl.when(z - d >= 0)
        def _():
            step(z - d, -1)

        @pl.when(z + d < lines)
        def _():
            step(z + d, 1)

    line_step(z, True, True, False)
    for d in range(1, lines):
        each(d, lambda k, sign: line_step(k, sign < 0, sign > 0, True))
        each(d - 1, lambda k, sign: side_step(k))
    each(lines - 1, lambda k, sign: side_step(k))
    for d in range(lines):
        each(d, lambda k, sign: diag_step(k))

    give.wait_send()
    for k in range(lines):
        to_x(k).wait_send()
        to_y(k).wait_send()
        diag_x(k).wait_send()
        diag_y(k).wait_send()

        @pl.when((k <= z) & has_above)
        def _():
            up(k).wait_send()

        @pl.when((k >= z) & has_below)
        def _():
            down(k).wait_send()
    for c in range(4 * lines):
        to_core(c).wait()


def shrink_kernel(steps, mine_ref, other_ref, out_ref, shrinkage_ref, mean_ref, cols, cols_other, narrow, scalars):
    step = pl.program_id(0)
    scen = lax.axis_index("scen")
    fac = lax.axis_index("fac")
    blocks, rows, half = mine_ref.shape
    total_rows = blocks * rows
    factors = 2 * half
    width = narrow.shape[0]
    tall = out_ref.shape[0]
    per_half = half // width
    in_mine = scen // per_half == fac
    offset = (scen % per_half) * width

    @pl.when(step == 0)
    def _():
        chunk = 512

        def centre(src, dst, i, mean_out):
            at = pl.ds(pl.multiple_of(i * chunk, chunk), chunk)
            total = src[0, :, at].astype(F32)
            for j in range(1, blocks):
                total = total + src[j, :, at].astype(F32)
            mean = jnp.sum(total, axis=0, keepdims=True) / total_rows
            if mean_out is not None:
                mean_out[:, at] = mean
            for j in range(0, blocks, 2):
                pair = src[pl.ds(j, 2), :, at].astype(F32).reshape(2 * rows, chunk)
                dst[pl.ds(j * rows, 2 * rows), at] = (pair - mean).astype(BF16)

        @pl.loop(0, half // chunk)
        def _(i):
            centre(mine_ref, cols, i, mean_ref)
            centre(other_ref, cols_other, i, None)

        at = pl.ds(pl.multiple_of(offset, width), width)

        @pl.when(in_mine)
        def _():
            narrow[...] = cols[:, at].T

        @pl.when(jnp.logical_not(in_mine))
        def _():
            narrow[...] = cols_other[:, at].T

        across = (((1,), (1,)), ((), ()))
        gram = lax.dot_general(cols[...], cols[...], across, preferred_element_type=F32)
        gram = gram + lax.dot_general(cols_other[...], cols_other[...], across, preferred_element_type=F32)
        on_diag = lax.broadcasted_iota(jnp.int32, gram.shape, 0) == lax.broadcasted_iota(jnp.int32, gram.shape, 1)
        gram_sq = gram * gram

        def total_of(v):
            return jnp.sum(jnp.sum(v, axis=0, keepdims=True), axis=1, keepdims=True)

        trace_total = total_of(jnp.where(on_diag, gram, 0.0))
        fourth_total = total_of(jnp.where(on_diag, gram_sq, 0.0))
        cov_sq = total_of(gram_sq) / (total_rows * total_rows)
        mu_scale = trace_total / (total_rows * factors)
        spread = (cov_sq - factors * mu_scale * mu_scale) / factors
        norm_sq = factors * (spread + mu_scale * mu_scale)
        beta_value = (fourth_total / total_rows - norm_sq) / (factors * total_rows)
        shrinkage = beta_value / spread
        shrinkage_ref[...] = shrinkage
        scalars[0:1, :] = jnp.broadcast_to((1.0 - shrinkage) / total_rows, (1, 128))
        scalars[1:2, :] = jnp.broadcast_to(shrinkage * mu_scale, (1, 128))

    scale = scalars[0:1, 0:1]
    left = narrow[pl.ds(pl.multiple_of(step * tall, tall), tall), :]
    piece = 1024
    for i in range(half // piece):
        at = pl.ds(i * piece, piece)
        out_ref[:, at] = jnp.dot(left, cols[:, at], preferred_element_type=F32) * scale

    @pl.when(in_mine)
    def _():
        at = pl.ds(pl.multiple_of(offset + step * tall, tall), tall)
        eye = lax.broadcasted_iota(jnp.int32, (tall, tall), 0) == lax.broadcasted_iota(jnp.int32, (tall, tall), 1)
        out_ref[:, at] = out_ref[:, at] + jnp.where(eye, scalars[1:2, 0:1], 0.0)


def on_chip_pairs(scenarios):
    rows, factors = scenarios.shape
    scen_size = lax.axis_size("scen")
    fac_size = lax.axis_size("fac")
    lines = scen_size // 4
    half = factors // fac_size
    width = factors // scen_size
    vmem = pl.BlockSpec(memory_space=pltpu.VMEM)
    held = pltpu.VMEM((scen_size, 2, rows, half), BF16)
    dma = pltpu.SemaphoreType.DMA
    mine, other = pl.pallas_call(
        functools.partial(gather_kernel, lines),
        out_shape=(held, held),
        in_specs=[vmem],
        out_specs=(vmem, vmem),
        scratch_shapes=[
            dma((1,)),
            dma((2, 1)),
            dma((3, lines)),
            dma((2, lines)),
            dma((2, lines)),
            dma((2, 2 * lines)),
            dma((2, scen_size)),
        ],
        compiler_params=pltpu.CompilerParams(collective_id=0, has_side_effects=True, vmem_limit_bytes=2**24),
        name="gather_rows",
    )(scenarios)
    mine = mine.reshape(2 * scen_size, rows, half)
    other = other.reshape(2 * scen_size, rows, half)
    total_rows = 2 * scen_size * rows
    tall = 128
    steps = width // tall
    shrunk, shrinkage, mean_block = pl.pallas_call(
        functools.partial(shrink_kernel, steps),
        grid=(steps,),
        out_shape=(
            jax.ShapeDtypeStruct((width, half), F32),
            jax.ShapeDtypeStruct((1, 1), F32),
            jax.ShapeDtypeStruct((1, half), F32),
        ),
        in_specs=[vmem, vmem],
        out_specs=(
            pl.BlockSpec((tall, half), lambda i: (i, 0)),
            pl.BlockSpec((1, 1), lambda i: (0, 0)),
            pl.BlockSpec((1, half), lambda i: (0, 0)),
        ),
        scratch_shapes=[
            pltpu.VMEM((total_rows, half), BF16),
            pltpu.VMEM((total_rows, half), BF16),
            pltpu.VMEM((width, total_rows), BF16),
            pltpu.VMEM((8, 128), F32),
        ],
        compiler_params=pltpu.CompilerParams(dimension_semantics=("arbitrary",), vmem_limit_bytes=2**25),
        name="shrink_rows",
    )(mine, other)
    return shrunk, shrinkage.reshape(()), mean_block.reshape(half)


def on_device(scenarios):
    row_count = scenarios.shape[0]
    factors = scenarios.shape[1]
    scen_size = lax.axis_size("scen")
    fac_size = lax.axis_size("fac")
    total_rows = row_count * scen_size * fac_size
    group_width = factors // scen_size
    block_width = factors // fac_size
    owner_idx = lax.axis_index("scen")
    block_idx = lax.axis_index("fac")
    col_total = lax.psum(jnp.sum(scenarios.astype(jnp.float32), axis=0), ("scen", "fac"))
    col_mean = col_total / total_rows
    centered = (scenarios.astype(jnp.float32) - col_mean).astype(jnp.bfloat16)
    as_float = centered.astype(jnp.float32)
    squared = jnp.sum(as_float * as_float, axis=1)
    trace_part = jnp.sum(squared)
    fourth_part = jnp.sum(squared * squared)
    trace_total, fourth_total = lax.psum((trace_part, fourth_part), ("scen", "fac"))
    contract = (((0,), (0,)), ((), ()))
    local_rows = lax.all_gather(centered, "fac", axis=0, tiled=True)
    narrow_all = lax.all_to_all(local_rows, "scen", split_axis=1, concat_axis=0, tiled=True)
    wide_cols = lax.dynamic_slice_in_dim(local_rows, block_idx * block_width, block_width, 1)
    summed = lax.dot_general(
        narrow_all,
        lax.all_gather(wide_cols, "scen", axis=0, tiled=True),
        contract,
        preferred_element_type=jnp.float32,
    )
    covariance = summed / total_rows
    row_index = owner_idx * group_width + lax.broadcasted_iota(
        jnp.int32, (group_width, block_width), 0
    )
    col_index = block_idx * block_width + lax.broadcasted_iota(
        jnp.int32, (group_width, block_width), 1
    )
    diag_mask = (row_index == col_index).astype(jnp.float32)
    mu_scale = trace_total / (total_rows * factors)
    distance = covariance - mu_scale * diag_mask
    frob_sum = lax.psum(jnp.sum(distance * distance), ("scen", "fac"))
    spread = frob_sum / factors
    norm_sq = factors * (spread + mu_scale * mu_scale)
    beta_value = (fourth_total / total_rows - norm_sq) / (factors * total_rows)
    shrinkage = beta_value / spread
    shrunk = (1.0 - shrinkage) * covariance + shrinkage * mu_scale * diag_mask
    mean_block = lax.dynamic_slice_in_dim(col_mean, block_idx * block_width, block_width, 0)
    return (shrunk, shrinkage, mean_block)


def solution(mesh):
    pairs = mesh.shape["fac"] == 2 and mesh.shape["scen"] % 4 == 0

    def step(scenarios):
        rows, factors = scenarios.shape
        width = factors // lax.axis_size("scen")
        gathered = rows * lax.axis_size("scen") * factors * 2 * scenarios.dtype.itemsize
        if pairs and rows == 8 and width % 128 == 0 and (factors // 2) % 1024 == 0 and gathered <= 2**23:
            return on_chip_pairs(scenarios)
        return on_device(scenarios)

    return jax.shard_map(
        step,
        mesh=mesh,
        in_specs=(P(("scen", "fac"), None),),
        out_specs=(P("scen", "fac"), P(), P("fac")),
        check_vma=False,
    )
```

```python
import functools

import jax
import jax.numpy as jnp
from jax import lax
from jax.experimental import pallas as pl
from jax.experimental.pallas import tpu as pltpu
from jax.sharding import PartitionSpec as P

MESH = pl.DeviceIdType.MESH
F32 = jnp.float32
BF16 = jnp.bfloat16


def gather_kernel(lines, rows_ref, mine_ref, other_ref, local_sem, pair_sems, z_sems, x_sems, y_sems, d_sems, line_sems, core_sems):
    reach = lines // 2
    scen = lax.axis_index("scen")
    fac = lax.axis_index("fac")
    z, y, x = scen // 4, (scen // 2) % 2, scen % 2
    half = mine_ref.shape[-1]
    mid = half // 2

    def chip(k, yy, xx):
        return k * 4 + yy * 2 + xx

    x_next = (chip(z, y, 1 - x), fac)
    y_next = (chip(z, 1 - y, x), fac)
    partner = (scen, 1 - fac)
    above = (chip(jnp.minimum(z + 1, lines - 1), y, x), fac)
    below = (chip(jnp.maximum(z - 1, 0), y, x), fac)
    has_above = z < lines - 1
    has_below = z > 0

    barrier = pltpu.get_barrier_semaphore()
    for device in (x_next, y_next, partner):
        pl.semaphore_signal(barrier, inc=1, device_id=device, device_id_type=MESH)

    @pl.when(has_above)
    def _():
        pl.semaphore_signal(barrier, inc=1, device_id=above, device_id_type=MESH)

    @pl.when(has_below)
    def _():
        pl.semaphore_signal(barrier, inc=1, device_id=below, device_id_type=MESH)

    pl.semaphore_wait(barrier, 3 + has_above.astype(jnp.int32) + has_below.astype(jnp.int32))

    def copy(ref, sems, i, device, sender=0):
        return pltpu.make_async_remote_copy(
            src_ref=ref,
            dst_ref=ref,
            send_sem=sems.at[sender, i],
            recv_sem=sems.at[1, i],
            device_id=device,
            device_id_type=MESH,
        )

    def core_of(i):
        return fac if i == 0 else 1 - fac

    def part(k, yy, xx, i):
        return mine_ref.at[chip(k, yy, xx), core_of(i)]

    def up(k, i):
        return copy(part(k, y, x, i), z_sems, 2 * k + i, above)

    def down(k, i):
        return copy(part(k, y, x, i), z_sems, 2 * k + i, below, 2)

    def to_x(k, i):
        return copy(part(k, y, x, i), x_sems, 2 * k + i, x_next)

    def to_y(k, i):
        return copy(part(k, y, x, i), y_sems, 2 * k + i, y_next)

    def diag_x(k):
        return copy(part(k, 1 - y, x, 0), d_sems, 2 * k, x_next)

    def diag_y(k):
        return copy(part(k, y, 1 - x, 1), d_sems, 2 * k + 1, y_next)

    def diag_up(k, i):
        return copy(part(k, 1 - y, 1 - x, i), line_sems, 2 * k + i, above)

    def diag_down(k, i):
        return copy(part(k, 1 - y, 1 - x, i), line_sems, 2 * k + i, below, 2)

    def to_core(c, j):
        return pltpu.make_async_remote_copy(
            src_ref=mine_ref.at[c, j],
            dst_ref=other_ref.at[c, j],
            send_sem=core_sems.at[0, 2 * c + j],
            recv_sem=core_sems.at[1, 2 * c + j],
            device_id=partner,
            device_id_type=MESH,
        )

    def start_if(condition, transfer):
        @pl.when(condition)
        def _():
            transfer.start()

    def line_step(k, sign, i):
        if sign:
            up(k, i).wait_recv()
        to_x(k, i).start()
        to_y(k, i).start()
        if sign <= 0:
            start_if(has_above, up(k, i))
        if sign >= 0:
            start_if(has_below, down(k, i))
        to_core(chip(k, y, x), core_of(i)).start()

    def side_step(k, crosses, i):
        to_x(k, i).wait_recv()
        if crosses and i == 1:
            diag_y(k).start()
        to_core(chip(k, y, 1 - x), core_of(i)).start()
        to_y(k, i).wait_recv()
        if crosses and i == 0:
            diag_x(k).start()
        to_core(chip(k, 1 - y, x), core_of(i)).start()

    def diag_step(k, sign, d, i):
        if d == 0 or d > reach:
            (diag_x, diag_y)[i](k).wait_recv()
        else:
            diag_up(k, i).wait_recv()
        if d < reach:
            if sign <= 0:
                start_if(has_above, diag_up(k, i))
            if sign >= 0:
                start_if(has_below, diag_down(k, i))
        to_core(chip(k, 1 - y, 1 - x), core_of(i)).start()

    def each(d, step):
        for i in range(2):
            if d == 0:
                step(z, 0, i)
                continue

            @pl.when(z - d >= 0)
            def _():
                step(z - d, -1, i)

            @pl.when(z + d < lines)
            def _():
                step(z + d, 1, i)

    def line(d):
        each(d, line_step)

    def side(d):
        each(d, lambda k, sign, i: side_step(k, d == 0 or d > reach, i))

    def diag(d):
        each(d, lambda k, sign, i: diag_step(k, sign, d, i))

    keep = pltpu.make_async_copy(
        rows_ref.at[:, pl.ds(pl.multiple_of(fac * half, half), half)], mine_ref.at[scen, fac], local_sem.at[0]
    )
    keep.start()
    give = pltpu.make_async_remote_copy(
        src_ref=rows_ref.at[:, pl.ds(pl.multiple_of((1 - fac) * half, half), half)],
        dst_ref=mine_ref.at[scen, fac],
        send_sem=pair_sems.at[0, 0],
        recv_sem=pair_sems.at[1, 0],
        device_id=partner,
        device_id_type=MESH,
    )
    give.start()
    keep.wait()
    line_step(z, 0, 0)
    give.wait_recv()
    line_step(z, 0, 1)
    for d in range(1, lines):
        line(d)
        if d >= 2:
            diag(d - 2)
        side(d - 1)
    if lines >= 2:
        diag(lines - 2)
    side(lines - 1)
    diag(lines - 1)

    give.wait_send()

    def sent_if(condition, *transfers):
        @pl.when(condition)
        def _():
            for transfer in transfers:
                transfer.wait_send()

    for k in range(lines):
        for i in range(2):
            to_x(k, i).wait_send()
            to_y(k, i).wait_send()
            sent_if((k <= z) & has_above, up(k, i))
            sent_if((k >= z) & has_below, down(k, i))
            sent_if((k <= z) & (k > z - reach) & has_above, diag_up(k, i))
            sent_if((k >= z) & (k < z + reach) & has_below, diag_down(k, i))
        sent_if((k == z) | (k > z + reach) | (k < z - reach), diag_x(k), diag_y(k))
    for c in range(4 * lines):
        for j in range(2):
            to_core(c, j).wait()


def shrink_kernel(steps, mine_ref, other_ref, out_ref, shrinkage_ref, mean_ref, cols, cols_other, narrow, scalars):
    step = pl.program_id(0)
    scen = lax.axis_index("scen")
    fac = lax.axis_index("fac")
    blocks, rows, half = mine_ref.shape
    total_rows = blocks * rows
    factors = 2 * half
    width = narrow.shape[0]
    tall = out_ref.shape[0]
    per_half = half // width
    in_mine = scen // per_half == fac
    offset = (scen % per_half) * width

    @pl.when(step == 0)
    def _():
        chunk = 512

        def centre(src, dst, i, mean_out):
            at = pl.ds(pl.multiple_of(i * chunk, chunk), chunk)
            total = src[0, :, at].astype(F32)
            for j in range(1, blocks):
                total = total + src[j, :, at].astype(F32)
            mean = jnp.sum(total, axis=0, keepdims=True) / total_rows
            if mean_out is not None:
                mean_out[:, at] = mean
            for j in range(0, blocks, 2):
                pair = src[pl.ds(j, 2), :, at].astype(F32).reshape(2 * rows, chunk)
                dst[pl.ds(j * rows, 2 * rows), at] = (pair - mean).astype(BF16)

        @pl.loop(0, half // chunk)
        def _(i):
            centre(mine_ref, cols, i, mean_ref)
            centre(other_ref, cols_other, i, None)

        at = pl.ds(pl.multiple_of(offset, width), width)

        @pl.when(in_mine)
        def _():
            narrow[...] = cols[:, at].T

        @pl.when(jnp.logical_not(in_mine))
        def _():
            narrow[...] = cols_other[:, at].T

        across = (((1,), (1,)), ((), ()))
        gram = lax.dot_general(cols[...], cols[...], across, preferred_element_type=F32)
        gram = gram + lax.dot_general(cols_other[...], cols_other[...], across, preferred_element_type=F32)
        on_diag = lax.broadcasted_iota(jnp.int32, gram.shape, 0) == lax.broadcasted_iota(jnp.int32, gram.shape, 1)
        gram_sq = gram * gram

        def total_of(v):
            return jnp.sum(jnp.sum(v, axis=0, keepdims=True), axis=1, keepdims=True)

        trace_total = total_of(jnp.where(on_diag, gram, 0.0))
        fourth_total = total_of(jnp.where(on_diag, gram_sq, 0.0))
        cov_sq = total_of(gram_sq) / (total_rows * total_rows)
        mu_scale = trace_total / (total_rows * factors)
        spread = (cov_sq - factors * mu_scale * mu_scale) / factors
        norm_sq = factors * (spread + mu_scale * mu_scale)
        beta_value = (fourth_total / total_rows - norm_sq) / (factors * total_rows)
        shrinkage = beta_value / spread
        shrinkage_ref[...] = shrinkage
        scalars[0:1, :] = jnp.broadcast_to((1.0 - shrinkage) / total_rows, (1, 128))
        scalars[1:2, :] = jnp.broadcast_to(shrinkage * mu_scale, (1, 128))

    scale = scalars[0:1, 0:1]
    left = narrow[pl.ds(pl.multiple_of(step * tall, tall), tall), :]
    piece = 1024
    for i in range(half // piece):
        at = pl.ds(i * piece, piece)
        out_ref[:, at] = jnp.dot(left, cols[:, at], preferred_element_type=F32) * scale

    @pl.when(in_mine)
    def _():
        at = pl.ds(pl.multiple_of(offset + step * tall, tall), tall)
        eye = lax.broadcasted_iota(jnp.int32, (tall, tall), 0) == lax.broadcasted_iota(jnp.int32, (tall, tall), 1)
        out_ref[:, at] = out_ref[:, at] + jnp.where(eye, scalars[1:2, 0:1], 0.0)


def on_chip_pairs(scenarios):
    rows, factors = scenarios.shape
    scen_size = lax.axis_size("scen")
    fac_size = lax.axis_size("fac")
    lines = scen_size // 4
    half = factors // fac_size
    width = factors // scen_size
    vmem = pl.BlockSpec(memory_space=pltpu.VMEM)
    held = pltpu.VMEM((scen_size, 2, rows, half), BF16)
    dma = pltpu.SemaphoreType.DMA
    mine, other = pl.pallas_call(
        functools.partial(gather_kernel, lines),
        out_shape=(held, held),
        in_specs=[vmem],
        out_specs=(vmem, vmem),
        scratch_shapes=[
            dma((1,)),
            dma((2, 1)),
            dma((3, 2 * lines)),
            dma((2, 2 * lines)),
            dma((2, 2 * lines)),
            dma((2, 2 * lines)),
            dma((3, 2 * lines)),
            dma((2, 2 * scen_size)),
        ],
        compiler_params=pltpu.CompilerParams(collective_id=0, has_side_effects=True, vmem_limit_bytes=2**24),
        name="gather_rows",
    )(scenarios)
    mine = mine.reshape(2 * scen_size, rows, half)
    other = other.reshape(2 * scen_size, rows, half)
    total_rows = 2 * scen_size * rows
    tall = 128
    steps = width // tall
    shrunk, shrinkage, mean_block = pl.pallas_call(
        functools.partial(shrink_kernel, steps),
        grid=(steps,),
        out_shape=(
            jax.ShapeDtypeStruct((width, half), F32),
            jax.ShapeDtypeStruct((1, 1), F32),
            jax.ShapeDtypeStruct((1, half), F32),
        ),
        in_specs=[vmem, vmem],
        out_specs=(
            pl.BlockSpec((tall, half), lambda i: (i, 0)),
            pl.BlockSpec((1, 1), lambda i: (0, 0)),
            pl.BlockSpec((1, half), lambda i: (0, 0)),
        ),
        scratch_shapes=[
            pltpu.VMEM((total_rows, half), BF16),
            pltpu.VMEM((total_rows, half), BF16),
            pltpu.VMEM((width, total_rows), BF16),
            pltpu.VMEM((8, 128), F32),
        ],
        compiler_params=pltpu.CompilerParams(dimension_semantics=("arbitrary",), vmem_limit_bytes=2**25),
        name="shrink_rows",
    )(mine, other)
    return shrunk, shrinkage.reshape(()), mean_block.reshape(half)


def on_device(scenarios):
    row_count = scenarios.shape[0]
    factors = scenarios.shape[1]
    scen_size = lax.axis_size("scen")
    fac_size = lax.axis_size("fac")
    total_rows = row_count * scen_size * fac_size
    group_width = factors // scen_size
    block_width = factors // fac_size
    owner_idx = lax.axis_index("scen")
    block_idx = lax.axis_index("fac")
    col_total = lax.psum(jnp.sum(scenarios.astype(jnp.float32), axis=0), ("scen", "fac"))
    col_mean = col_total / total_rows
    centered = (scenarios.astype(jnp.float32) - col_mean).astype(jnp.bfloat16)
    as_float = centered.astype(jnp.float32)
    squared = jnp.sum(as_float * as_float, axis=1)
    trace_part = jnp.sum(squared)
    fourth_part = jnp.sum(squared * squared)
    trace_total, fourth_total = lax.psum((trace_part, fourth_part), ("scen", "fac"))
    contract = (((0,), (0,)), ((), ()))
    local_rows = lax.all_gather(centered, "fac", axis=0, tiled=True)
    narrow_all = lax.all_to_all(local_rows, "scen", split_axis=1, concat_axis=0, tiled=True)
    wide_cols = lax.dynamic_slice_in_dim(local_rows, block_idx * block_width, block_width, 1)
    summed = lax.dot_general(
        narrow_all,
        lax.all_gather(wide_cols, "scen", axis=0, tiled=True),
        contract,
        preferred_element_type=jnp.float32,
    )
    covariance = summed / total_rows
    row_index = owner_idx * group_width + lax.broadcasted_iota(
        jnp.int32, (group_width, block_width), 0
    )
    col_index = block_idx * block_width + lax.broadcasted_iota(
        jnp.int32, (group_width, block_width), 1
    )
    diag_mask = (row_index == col_index).astype(jnp.float32)
    mu_scale = trace_total / (total_rows * factors)
    distance = covariance - mu_scale * diag_mask
    frob_sum = lax.psum(jnp.sum(distance * distance), ("scen", "fac"))
    spread = frob_sum / factors
    norm_sq = factors * (spread + mu_scale * mu_scale)
    beta_value = (fourth_total / total_rows - norm_sq) / (factors * total_rows)
    shrinkage = beta_value / spread
    shrunk = (1.0 - shrinkage) * covariance + shrinkage * mu_scale * diag_mask
    mean_block = lax.dynamic_slice_in_dim(col_mean, block_idx * block_width, block_width, 0)
    return (shrunk, shrinkage, mean_block)


def solution(mesh):
    pairs = mesh.shape["fac"] == 2 and mesh.shape["scen"] % 4 == 0

    def step(scenarios):
        rows, factors = scenarios.shape
        width = factors // lax.axis_size("scen")
        gathered = rows * lax.axis_size("scen") * factors * 2 * scenarios.dtype.itemsize
        if pairs and rows == 8 and width % 128 == 0 and (factors // 2) % 1024 == 0 and gathered <= 2**23:
            return on_chip_pairs(scenarios)
        return on_device(scenarios)

    return jax.shard_map(
        step,
        mesh=mesh,
        in_specs=(P(("scen", "fac"), None),),
        out_specs=(P("scen", "fac"), P(), P("fac")),
        check_vma=False,
    )
```

```python
import functools

import jax
import jax.numpy as jnp
from jax import lax
from jax.experimental import pallas as pl
from jax.experimental.pallas import tpu as pltpu
from jax.sharding import PartitionSpec as P

MESH = pl.DeviceIdType.MESH
F32 = jnp.float32
BF16 = jnp.bfloat16


def gather_kernel(lines, input_ref, mine_ref, other_ref, rows_ref, local_sem, pair_sems, z_sems, x_sems, y_sems, d_sems, line_sems, core_sems):
    reach = 1
    load = pltpu.make_async_copy(input_ref, rows_ref, local_sem.at[1])
    load.start()
    scen = lax.axis_index("scen")
    fac = lax.axis_index("fac")
    z, y, x = scen // 4, (scen // 2) % 2, scen % 2
    half = mine_ref.shape[-1]
    mid = half // 2

    def chip(k, yy, xx):
        return k * 4 + yy * 2 + xx

    x_next = (chip(z, y, 1 - x), fac)
    y_next = (chip(z, 1 - y, x), fac)
    partner = (scen, 1 - fac)
    above = (chip(jnp.minimum(z + 1, lines - 1), y, x), fac)
    below = (chip(jnp.maximum(z - 1, 0), y, x), fac)
    has_above = z < lines - 1
    has_below = z > 0

    barrier = pltpu.get_barrier_semaphore()
    for device in (x_next, y_next, partner):
        pl.semaphore_signal(barrier, inc=1, device_id=device, device_id_type=MESH)

    @pl.when(has_above)
    def _():
        pl.semaphore_signal(barrier, inc=1, device_id=above, device_id_type=MESH)

    @pl.when(has_below)
    def _():
        pl.semaphore_signal(barrier, inc=1, device_id=below, device_id_type=MESH)

    pl.semaphore_wait(barrier, 3 + has_above.astype(jnp.int32) + has_below.astype(jnp.int32))

    def copy(ref, sems, i, device, sender=0):
        return pltpu.make_async_remote_copy(
            src_ref=ref,
            dst_ref=ref,
            send_sem=sems.at[sender, i],
            recv_sem=sems.at[1, i],
            device_id=device,
            device_id_type=MESH,
        )

    def core_of(i):
        return fac if i == 0 else 1 - fac

    def part(k, yy, xx, i):
        return mine_ref.at[chip(k, yy, xx), core_of(i)]

    def up(k, i):
        return copy(part(k, y, x, i), z_sems, 2 * k + i, above)

    def down(k, i):
        return copy(part(k, y, x, i), z_sems, 2 * k + i, below, 2)

    def to_x(k, i):
        return copy(part(k, y, x, i), x_sems, 2 * k + i, x_next)

    def to_y(k, i):
        return copy(part(k, y, x, i), y_sems, 2 * k + i, y_next)

    def diag_x(k):
        return copy(part(k, 1 - y, x, 0), d_sems, 2 * k, x_next)

    def diag_y(k):
        return copy(part(k, y, 1 - x, 1), d_sems, 2 * k + 1, y_next)

    def diag_up(k, i):
        return copy(part(k, 1 - y, 1 - x, i), line_sems, 2 * k + i, above)

    def diag_down(k, i):
        return copy(part(k, 1 - y, 1 - x, i), line_sems, 2 * k + i, below, 2)

    def to_core(c, j):
        return pltpu.make_async_remote_copy(
            src_ref=mine_ref.at[c, j],
            dst_ref=other_ref.at[c, j],
            send_sem=core_sems.at[0, 2 * c + j],
            recv_sem=core_sems.at[1, 2 * c + j],
            device_id=partner,
            device_id_type=MESH,
        )

    def start_if(condition, transfer):
        @pl.when(condition)
        def _():
            transfer.start()

    def line_step(k, sign, i):
        if sign:
            up(k, i).wait_recv()
        to_x(k, i).start()
        to_y(k, i).start()
        if sign <= 0:
            start_if(has_above, up(k, i))
        if sign >= 0:
            start_if(has_below, down(k, i))
        to_core(chip(k, y, x), core_of(i)).start()

    def side_step(k, crosses, i):
        to_x(k, i).wait_recv()
        if crosses and i == 1:
            diag_y(k).start()
        to_core(chip(k, y, 1 - x), core_of(i)).start()
        to_y(k, i).wait_recv()
        if crosses and i == 0:
            diag_x(k).start()
        to_core(chip(k, 1 - y, x), core_of(i)).start()

    def diag_step(k, sign, d, i):
        if d == 0 or d > reach:
            (diag_x, diag_y)[i](k).wait_recv()
        else:
            diag_up(k, i).wait_recv()
        if d < reach:
            if sign <= 0:
                start_if(has_above, diag_up(k, i))
            if sign >= 0:
                start_if(has_below, diag_down(k, i))
        to_core(chip(k, 1 - y, 1 - x), core_of(i)).start()

    def each(d, step):
        for i in range(2):
            if d == 0:
                step(z, 0, i)
                continue

            @pl.when(z - d >= 0)
            def _():
                step(z - d, -1, i)

            @pl.when(z + d < lines)
            def _():
                step(z + d, 1, i)

    def line(d):
        each(d, line_step)

    def side(d):
        each(d, lambda k, sign, i: side_step(k, d == 0 or d > reach, i))

    def diag(d):
        each(d, lambda k, sign, i: diag_step(k, sign, d, i))

    load.wait()
    keep = pltpu.make_async_copy(
        rows_ref.at[:, pl.ds(pl.multiple_of(fac * half, half), half)], mine_ref.at[scen, fac], local_sem.at[0]
    )
    keep.start()
    give = pltpu.make_async_remote_copy(
        src_ref=rows_ref.at[:, pl.ds(pl.multiple_of((1 - fac) * half, half), half)],
        dst_ref=mine_ref.at[scen, fac],
        send_sem=pair_sems.at[0, 0],
        recv_sem=pair_sems.at[1, 0],
        device_id=partner,
        device_id_type=MESH,
    )
    give.start()
    keep.wait()
    line_step(z, 0, 0)
    give.wait_recv()
    line_step(z, 0, 1)
    for d in range(1, lines):
        line(d)
        if d >= 2:
            diag(d - 2)
        side(d - 1)
    if lines >= 2:
        diag(lines - 2)
    side(lines - 1)
    diag(lines - 1)

    give.wait_send()

    def sent_if(condition, *transfers):
        @pl.when(condition)
        def _():
            for transfer in transfers:
                transfer.wait_send()

    for k in range(lines):
        for i in range(2):
            to_x(k, i).wait_send()
            to_y(k, i).wait_send()
            sent_if((k <= z) & has_above, up(k, i))
            sent_if((k >= z) & has_below, down(k, i))
            sent_if((k <= z) & (k > z - reach) & has_above, diag_up(k, i))
            sent_if((k >= z) & (k < z + reach) & has_below, diag_down(k, i))
        sent_if((k == z) | (k > z + reach) | (k < z - reach), diag_x(k), diag_y(k))
    for c in range(4 * lines):
        for j in range(2):
            to_core(c, j).wait()


def shrink_kernel(steps, mine_ref, other_ref, out_ref, shrinkage_ref, mean_ref, cols, cols_other, narrow, scalars):
    step = pl.program_id(0)
    scen = lax.axis_index("scen")
    fac = lax.axis_index("fac")
    blocks, rows, half = mine_ref.shape
    total_rows = blocks * rows
    factors = 2 * half
    width = narrow.shape[0]
    tall = out_ref.shape[0]
    per_half = half // width
    in_mine = scen // per_half == fac
    offset = (scen % per_half) * width

    @pl.when(step == 0)
    def _():
        chunk = 512

        def centre(src, dst, i, mean_out):
            at = pl.ds(pl.multiple_of(i * chunk, chunk), chunk)
            total = src[0, :, at].astype(F32)
            for j in range(1, blocks):
                total = total + src[j, :, at].astype(F32)
            mean = jnp.sum(total, axis=0, keepdims=True) / total_rows
            if mean_out is not None:
                mean_out[:, at] = mean
            for j in range(0, blocks, 2):
                pair = src[pl.ds(j, 2), :, at].astype(F32).reshape(2 * rows, chunk)
                dst[pl.ds(j * rows, 2 * rows), at] = (pair - mean).astype(BF16)

        @pl.loop(0, half // chunk)
        def _(i):
            centre(mine_ref, cols, i, mean_ref)
            centre(other_ref, cols_other, i, None)

        at = pl.ds(pl.multiple_of(offset, width), width)

        @pl.when(in_mine)
        def _():
            narrow[...] = cols[:, at].T

        @pl.when(jnp.logical_not(in_mine))
        def _():
            narrow[...] = cols_other[:, at].T

        across = (((1,), (1,)), ((), ()))
        gram = lax.dot_general(cols[...], cols[...], across, preferred_element_type=F32)
        gram = gram + lax.dot_general(cols_other[...], cols_other[...], across, preferred_element_type=F32)
        on_diag = lax.broadcasted_iota(jnp.int32, gram.shape, 0) == lax.broadcasted_iota(jnp.int32, gram.shape, 1)
        gram_sq = gram * gram

        def total_of(v):
            return jnp.sum(jnp.sum(v, axis=0, keepdims=True), axis=1, keepdims=True)

        trace_total = total_of(jnp.where(on_diag, gram, 0.0))
        fourth_total = total_of(jnp.where(on_diag, gram_sq, 0.0))
        cov_sq = total_of(gram_sq) / (total_rows * total_rows)
        mu_scale = trace_total / (total_rows * factors)
        spread = (cov_sq - factors * mu_scale * mu_scale) / factors
        norm_sq = factors * (spread + mu_scale * mu_scale)
        beta_value = (fourth_total / total_rows - norm_sq) / (factors * total_rows)
        shrinkage = beta_value / spread
        shrinkage_ref[...] = shrinkage
        scalars[0:1, :] = jnp.broadcast_to((1.0 - shrinkage) / total_rows, (1, 128))
        scalars[1:2, :] = jnp.broadcast_to(shrinkage * mu_scale, (1, 128))

    scale = scalars[0:1, 0:1]
    left = narrow[pl.ds(pl.multiple_of(step * tall, tall), tall), :]
    piece = 1024
    for i in range(half // piece):
        at = pl.ds(i * piece, piece)
        out_ref[:, at] = jnp.dot(left, cols[:, at], preferred_element_type=F32) * scale

    @pl.when(in_mine)
    def _():
        at = pl.ds(pl.multiple_of(offset + step * tall, tall), tall)
        eye = lax.broadcasted_iota(jnp.int32, (tall, tall), 0) == lax.broadcasted_iota(jnp.int32, (tall, tall), 1)
        out_ref[:, at] = out_ref[:, at] + jnp.where(eye, scalars[1:2, 0:1], 0.0)


def on_chip_pairs(scenarios):
    rows, factors = scenarios.shape
    scen_size = lax.axis_size("scen")
    fac_size = lax.axis_size("fac")
    lines = scen_size // 4
    half = factors // fac_size
    width = factors // scen_size
    vmem = pl.BlockSpec(memory_space=pltpu.VMEM)
    held = pltpu.VMEM((scen_size, 2, rows, half), BF16)
    dma = pltpu.SemaphoreType.DMA
    mine, other = pl.pallas_call(
        functools.partial(gather_kernel, lines),
        out_shape=(held, held),
        in_specs=[pl.BlockSpec(memory_space=pltpu.HBM)],
        out_specs=(vmem, vmem),
        scratch_shapes=[
            pltpu.VMEM((rows, factors), BF16),
            dma((2,)),
            dma((2, 1)),
            dma((3, 2 * lines)),
            dma((2, 2 * lines)),
            dma((2, 2 * lines)),
            dma((2, 2 * lines)),
            dma((3, 2 * lines)),
            dma((2, 2 * scen_size)),
        ],
        compiler_params=pltpu.CompilerParams(collective_id=0, has_side_effects=True, vmem_limit_bytes=2**24),
        name="gather_rows",
    )(scenarios)
    mine = mine.reshape(2 * scen_size, rows, half)
    other = other.reshape(2 * scen_size, rows, half)
    total_rows = 2 * scen_size * rows
    tall = 128
    steps = width // tall
    shrunk, shrinkage, mean_block = pl.pallas_call(
        functools.partial(shrink_kernel, steps),
        grid=(steps,),
        out_shape=(
            jax.ShapeDtypeStruct((width, half), F32),
            jax.ShapeDtypeStruct((1, 1), F32),
            jax.ShapeDtypeStruct((1, half), F32),
        ),
        in_specs=[vmem, vmem],
        out_specs=(
            pl.BlockSpec((tall, half), lambda i: (i, 0)),
            pl.BlockSpec((1, 1), lambda i: (0, 0)),
            pl.BlockSpec((1, half), lambda i: (0, 0)),
        ),
        scratch_shapes=[
            pltpu.VMEM((total_rows, half), BF16),
            pltpu.VMEM((total_rows, half), BF16),
            pltpu.VMEM((width, total_rows), BF16),
            pltpu.VMEM((8, 128), F32),
        ],
        compiler_params=pltpu.CompilerParams(dimension_semantics=("arbitrary",), vmem_limit_bytes=2**25),
        name="shrink_rows",
    )(mine, other)
    return shrunk, shrinkage.reshape(()), mean_block.reshape(half)


def on_device(scenarios):
    row_count = scenarios.shape[0]
    factors = scenarios.shape[1]
    scen_size = lax.axis_size("scen")
    fac_size = lax.axis_size("fac")
    total_rows = row_count * scen_size * fac_size
    group_width = factors // scen_size
    block_width = factors // fac_size
    owner_idx = lax.axis_index("scen")
    block_idx = lax.axis_index("fac")
    col_total = lax.psum(jnp.sum(scenarios.astype(jnp.float32), axis=0), ("scen", "fac"))
    col_mean = col_total / total_rows
    centered = (scenarios.astype(jnp.float32) - col_mean).astype(jnp.bfloat16)
    as_float = centered.astype(jnp.float32)
    squared = jnp.sum(as_float * as_float, axis=1)
    trace_part = jnp.sum(squared)
    fourth_part = jnp.sum(squared * squared)
    trace_total, fourth_total = lax.psum((trace_part, fourth_part), ("scen", "fac"))
    contract = (((0,), (0,)), ((), ()))
    local_rows = lax.all_gather(centered, "fac", axis=0, tiled=True)
    narrow_all = lax.all_to_all(local_rows, "scen", split_axis=1, concat_axis=0, tiled=True)
    wide_cols = lax.dynamic_slice_in_dim(local_rows, block_idx * block_width, block_width, 1)
    summed = lax.dot_general(
        narrow_all,
        lax.all_gather(wide_cols, "scen", axis=0, tiled=True),
        contract,
        preferred_element_type=jnp.float32,
    )
    covariance = summed / total_rows
    row_index = owner_idx * group_width + lax.broadcasted_iota(
        jnp.int32, (group_width, block_width), 0
    )
    col_index = block_idx * block_width + lax.broadcasted_iota(
        jnp.int32, (group_width, block_width), 1
    )
    diag_mask = (row_index == col_index).astype(jnp.float32)
    mu_scale = trace_total / (total_rows * factors)
    distance = covariance - mu_scale * diag_mask
    frob_sum = lax.psum(jnp.sum(distance * distance), ("scen", "fac"))
    spread = frob_sum / factors
    norm_sq = factors * (spread + mu_scale * mu_scale)
    beta_value = (fourth_total / total_rows - norm_sq) / (factors * total_rows)
    shrinkage = beta_value / spread
    shrunk = (1.0 - shrinkage) * covariance + shrinkage * mu_scale * diag_mask
    mean_block = lax.dynamic_slice_in_dim(col_mean, block_idx * block_width, block_width, 0)
    return (shrunk, shrinkage, mean_block)


def solution(mesh):
    pairs = mesh.shape["fac"] == 2 and mesh.shape["scen"] % 4 == 0

    def step(scenarios):
        rows, factors = scenarios.shape
        width = factors // lax.axis_size("scen")
        gathered = rows * lax.axis_size("scen") * factors * 2 * scenarios.dtype.itemsize
        if pairs and rows == 8 and width % 128 == 0 and (factors // 2) % 1024 == 0 and gathered <= 2**23:
            return on_chip_pairs(scenarios)
        return on_device(scenarios)

    return jax.shard_map(
        step,
        mesh=mesh,
        in_specs=(P(("scen", "fac"), None),),
        out_specs=(P("scen", "fac"), P(), P("fac")),
        check_vma=False,
    )
```
